32 devices in a mesh: gx: 2 (over y), gy: 4 (over z), gz: 4 (over x, core).
Axes of the slice: x: 2, y: 2, z: 4, core: 2. Of those that a mesh axis runs over, the one named last changes fastest.
Arguments:
- concentration: float32 [32, 256, 512], P('gx', 'gy', 'gz'), may hold values from -6 to 6
- speed: float32 [3, 32, 256, 512], P(None, 'gx', 'gy', 'gz'), may hold values from 0.1 to 1
- signs: int32 [3, 32, 256, 512], P(None, 'gx', 'gy', 'gz'), may hold values from 0 to 1
- diffusivity: float32 [32, 256, 512], P('gx', 'gy', 'gz'), may hold values from 0.02 to 0.12
- shear: int32 [1], replicated, may hold values from 0 to 255
Outputs:
- final_field: float32 [32, 256, 512], P('gx', 'gy', 'gz')
The draws below stay inside these ranges and needn't reach their ends.
All inputs are finite; a program needn't handle non-finite values.
Results may differ from the reference program's by a relative error of at most 0.00002.
Values sent between devices are 32-bit elements; how exact they have to be, the bound alone decides.
A program may use at most 64 MiB of HBM per device.

```python
import math
import jax
import jax.numpy as jnp

STEPS = 8
NX = 32
NY = 256
NZ = 512


def with_ends(values, rng, low, largest):
    shape = values.shape
    place = [jax.random.randint(jax.random.fold_in(rng, axis), (), 0, shape[axis]) for axis in range(len(shape))]
    values = values.at[tuple(place)].set(low)
    longest = shape.index(max(shape))
    place[longest] = (place[longest] + 1) % shape[longest]
    return values.at[tuple(place)].set(largest)


def level_of(rng, shape, shards, least, high):
    loudness, own = 1.0, jax.random.fold_in(rng, 6)
    for position, parts in shards:
        draws = jnp.exp(jax.random.uniform(jax.random.fold_in(own, position), (parts,), jnp.float32, least / len(shards), high / len(shards)))
        loudness = loudness * jnp.repeat(draws, shape[position] // parts).reshape([-1 if axis == position else 1 for axis in range(len(shape))])
    return loudness


def scatter_about(own_key, dims, width, limit, pieces=(), kind=jnp.bfloat16):
    entries = width * jax.random.normal(own_key, dims, jnp.float32)
    if pieces:
        entries = entries * level_of(own_key, dims, pieces, -0.22, 0.18)
    return jnp.clip(entries, -limit, limit).astype(kind)


def setup_inputs(seed: int = 0) -> dict:
    key_list = jax.random.split(jax.random.key(seed), 6)
    concentration = scatter_about(key_list[0], (NX, NY, NZ), 1.0, 6.0, ((0, 2), (1, 4), (2, 4)), jnp.float32)
    speed = jnp.clip(jnp.exp(math.log(1.0) - 2.3025851 * jax.random.uniform(key_list[1], (3, NX, NY, NZ), jnp.float32) ** level_of(key_list[1], (3, NX, NY, NZ), ((1, 2), (2, 4), (3, 4)), -0.2, 0.2)), 0.1, 1.0)
    signs = with_ends(jax.random.randint(key_list[2], (3, NX, NY, NZ), 0, 2), jax.random.fold_in(key_list[2], 1), 0, 1).astype(jnp.int32)
    diffusivity = jnp.clip(jnp.exp(math.log(0.12) - 1.7917595 * jax.random.uniform(key_list[3], (NX, NY, NZ), jnp.float32) ** level_of(key_list[3], (NX, NY, NZ), ((0, 2), (1, 4), (2, 4)), -0.2, 0.2)), 0.02, 0.12)
    shear = jax.random.randint(key_list[4], (1,), 0, NY).astype(jnp.int32)
    return {"concentration": concentration, "speed": speed, "signs": signs, "diffusivity": diffusivity, "shear": shear}


time_step = 0.25


def advance(field, neighbours, speed, signs, diffusivity):
    total = jnp.zeros_like(field)
    for axis_id in range(3):
        below, above = neighbours[axis_id]
        upwind = jnp.where(signs[axis_id] > 0, field - below, above - field)
        total = total + diffusivity * (above + below - 2.0 * field) - speed[axis_id] * upwind
    return field + time_step * total


def reference(concentration, speed, signs, diffusivity, shear):
    offset = shear[0]
    field = concentration
    for step in range(STEPS):
        lower = jnp.roll(field[-1], -offset, axis=0)
        upper = jnp.roll(field[0], offset, axis=0)
        x_minus = jnp.concatenate([lower[None], field[:-1]], axis=0)
        x_plus = jnp.concatenate([field[1:], upper[None]], axis=0)
        y_minus = jnp.roll(field, 1, axis=1)
        y_plus = jnp.roll(field, -1, axis=1)
        z_minus = jnp.roll(field, 1, axis=2)
        z_plus = jnp.roll(field, -1, axis=2)
        field = advance(field, ((x_minus, x_plus), (y_minus, y_plus), (z_minus, z_plus)), speed, signs, diffusivity)
    return field
```

```python
import functools

import jax
import jax.numpy as jnp
from jax import lax
from jax.experimental import pallas as pl
from jax.experimental.pallas import tpu as pltpu
from jax.sharding import PartitionSpec as P

STEPS = 8
time_step = 0.25
PAD = 8
MESH = pl.DeviceIdType.MESH


def kernel(
    hops, count_x, count_y, count_z,
    shear, conc, speed, signs, diff, out,
    field, coef, v_buf, s_buf, d_buf, low0, low1, high0, high1, y_out, y_in, z_out, z_in,
    load_sem, send_sem, recv_sem,
):
    nx, rows, lanes = conc.shape
    blocks = rows // 8
    span = 2 * nx
    per = lanes // span
    gx, gy, gz = (lax.axis_index(name) for name in ("gx", "gy", "gz"))
    low, high = (low0, low1), (high0, high1)
    first, last = gx == 0, gx == count_x - 1
    body_rows = pl.ds(PAD, rows)

    def at(x, y):
        return {"gx": x, "gy": lax.rem(y + 2 * count_y, count_y)}

    up = (
        at(jnp.where(last, 0, gx + 1), gy - jnp.where(last, hops, 0)),
        at(0, gy - hops - 1),
    )
    down = (
        at(jnp.where(first, count_x - 1, gx - 1), gy + jnp.where(first, hops + 1, 0)),
        at(count_x - 1, gy + hops),
    )
    before_y, after_y = at(gx, gy - 1), at(gx, gy + 1)
    before_z = {"gz": lax.rem(gz + count_z - 1, count_z)}
    after_z = {"gz": lax.rem(gz + 1, count_z)}

    def remote(p, role, source, target, device):
        return pltpu.make_async_remote_copy(
            src_ref=source, dst_ref=target,
            send_sem=send_sem.at[p, role], recv_sem=recv_sem.at[p, role],
            device_id=device, device_id_type=MESH,
        )

    def copies(p):
        top = field.at[p, nx - 1, body_rows]
        bottom = field.at[p, 0, body_rows]
        halves = (pl.ds(0, rows), pl.ds(rows, rows))
        return (
            remote(p, 0, top, low[p].at[halves[0]], up[0]),
            remote(p, 1, top, low[p].at[halves[1]], up[1]),
            remote(p, 2, bottom, high[p].at[halves[0]], down[0]),
            remote(p, 3, bottom, high[p].at[halves[1]], down[1]),
            remote(p, 4, y_out.at[p, 0], y_in.at[p, 1], before_y),
            remote(p, 5, y_out.at[p, 1], y_in.at[p, 0], after_y),
            remote(p, 6, z_out.at[p], z_in.at[p, 1], before_z),
            remote(p, 7, z_out.at[p], z_in.at[p, 0], after_z),
        )

    def send(p):
        c = copies(p)
        pl.when(last)(c[1].start)
        pl.when(first)(c[3].start)
        for role in (0, 2, 4, 5, 6, 7):
            c[role].start()

    lane = lax.broadcasted_iota(jnp.int32, (8, lanes), 1)
    even = lane % 2 == 0

    def turn(value, amount):
        return pltpu.roll(value, lax.rem(amount + 2 * lanes, lanes), 1)

    def pack(packed, block, x, value):
        spot = span * (block % per) + 2 * x
        moved = turn(value, spot + 1)
        group = block // per
        old = packed[group]
        new = jnp.where((lane == spot) | (lane == spot + 1), moved, old)
        return packed[:group] + (new,) + packed[group + 1 :]

    def put_edges(q, x, packed):
        y_out[q, 0, pl.ds(x, 1)] = field[q, x, pl.ds(PAD, 1)]
        y_out[q, 1, pl.ds(x, 1)] = field[q, x, pl.ds(PAD + rows - 1, 1)]

    def store_packed(q, packed):
        for group, value in enumerate(packed):
            z_out[q, group] = value

    groups = blocks // per
    nothing = tuple(jnp.zeros((8, lanes), jnp.float32) for _ in range(groups))

    loads = (
        pltpu.make_async_copy(conc, field.at[0, :, body_rows], load_sem.at[0]),
        pltpu.make_async_copy(diff, d_buf, load_sem.at[1]),
        pltpu.make_async_copy(speed, v_buf, load_sem.at[2]),
        pltpu.make_async_copy(signs, s_buf, load_sem.at[3]),
    )
    for load in loads:
        load.start()

    barrier = pltpu.get_barrier_semaphore()

    def greet(device):
        pl.semaphore_signal(barrier, inc=1, device_id=device, device_id_type=MESH)

    for device in (up[0], down[0], before_y, after_y, before_z, after_z):
        greet(device)
    pl.when(last)(lambda: greet(up[1]))
    pl.when(first)(lambda: greet(down[1]))
    pl.semaphore_wait(barrier, 6 + jnp.where(first | last, 1, 0))

    loads[0].wait()

    def first_pack(x, packed):
        for block in range(blocks):
            packed = pack(packed, block, x, field[0, x, pl.ds(PAD + 8 * block, 8)])
        put_edges(0, x, packed)
        return packed

    store_packed(0, lax.fori_loop(0, nx, first_pack, nothing))
    send(0)
    for load in loads[1:]:
        load.wait()

    def weigh(x, carry):
        d = time_step * d_buf[x]
        centre = 1.0 - 6.0 * d
        for axis in range(3):
            v = time_step * v_buf[axis, x]
            forward = s_buf[axis, x] > 0
            below = jnp.where(forward, v, 0.0)
            above = v - below
            coef[1 + 2 * axis, x] = d + below
            coef[2 + 2 * axis, x] = d - above
            centre = centre - below + above
        coef[0, x] = centre
        return carry

    lax.fori_loop(0, nx, weigh, 0)

    residue = lax.rem(shear[0], rows)
    low_start = jnp.where(first, residue, 0)
    high_start = jnp.where(last, rows - residue, 0)

    def step(p, more):
        q = 1 - p
        c = copies(p)
        for role in (4, 5, 6, 7):
            c[role].wait_recv()
        for x in range(nx):
            field[p, x, pl.ds(PAD - 1, 1)] = y_in[p, 0, pl.ds(x, 1)]
            field[p, x, pl.ds(PAD + rows, 1)] = y_in[p, 1, pl.ds(x, 1)]
        sides = tuple(
            jnp.where(even, z_in[p, 0, group], turn(z_in[p, 1, group], -2))
            for group in range(groups)
        )

        def plane(x, packed, lower, upper):
            for block in range(blocks):
                start = PAD + 8 * block
                part = pl.ds(8 * block, 8)
                here = field[p, x, pl.ds(start, 8)]
                side = turn(sides[block // per], -(span * (block % per) + 2 * x))
                z_minus = jnp.where(lane == 0, side, turn(here, 1))
                z_plus = jnp.where(lane == lanes - 1, side, turn(here, -1))
                total = (
                    (coef[0, x, part] * here + coef[1, x, part] * lower(block))
                    + (coef[2, x, part] * upper(block)
                       + coef[3, x, part] * field[p, x, pl.ds(start - 1, 8)])
                ) + (
                    (coef[4, x, part] * field[p, x, pl.ds(start + 1, 8)]
                     + coef[5, x, part] * z_minus)
                    + coef[6, x, part] * z_plus
                )
                field[q, x, pl.ds(start, 8)] = total
                packed = pack(packed, block, x, total)
            put_edges(q, x, packed)
            return packed

        def from_field(x):
            return lambda block: field[p, x, pl.ds(PAD + 8 * block, 8)]

        packed = lax.fori_loop(
            1, nx - 1,
            lambda x, packed: plane(x, packed, from_field(x - 1), from_field(x + 1)),
            nothing,
        )
        c[0].wait_recv()
        c[2].wait_recv()
        pl.when(first)(c[1].wait_recv)
        pl.when(last)(c[3].wait_recv)
        packed = plane(
            0, packed, lambda block: low[p][pl.ds(low_start + 8 * block, 8)], from_field(1)
        )
        packed = plane(
            nx - 1, packed, from_field(nx - 2),
            lambda block: high[p][pl.ds(high_start + 8 * block, 8)],
        )
        store_packed(q, packed)
        for role in (0, 2, 4, 5, 6, 7):
            c[role].wait_send()
        pl.when(last)(c[1].wait_send)
        pl.when(first)(c[3].wait_send)
        if more is None:
            send(q)
        else:
            pl.when(more)(lambda: send(q))

    def pair(t, carry):
        step(0, None)
        step(1, t < STEPS // 2 - 1)
        return carry

    lax.fori_loop(0, STEPS // 2, pair, 0)
    store = pltpu.make_async_copy(field.at[STEPS % 2, :, body_rows], out, load_sem.at[0])
    store.start()
    store.wait()


def run(hops, counts, shear, conc, speed, signs, diff):
    nx, rows, lanes = conc.shape
    f32 = jnp.float32
    groups = (rows // 8) // (lanes // (2 * nx))
    anywhere = pl.BlockSpec(memory_space=pl.ANY)
    return pl.pallas_call(
        functools.partial(kernel, hops, *counts),
        name=f"slide{hops}",
        out_shape=jax.ShapeDtypeStruct(conc.shape, f32),
        in_specs=[pl.BlockSpec(memory_space=pltpu.SMEM)] + [anywhere] * 4,
        out_specs=anywhere,
        scratch_shapes=[
            pltpu.VMEM((2, nx, rows + 2 * PAD, lanes), f32),
            pltpu.VMEM((7, nx, rows, lanes), f32),
            pltpu.VMEM((3, nx, rows, lanes), f32),
            pltpu.VMEM((3, nx, rows, lanes), jnp.int32),
            pltpu.VMEM((nx, rows, lanes), f32),
            pltpu.VMEM((2 * rows, lanes), f32),
            pltpu.VMEM((2 * rows, lanes), f32),
            pltpu.VMEM((2 * rows, lanes), f32),
            pltpu.VMEM((2 * rows, lanes), f32),
            pltpu.VMEM((2, 2, nx, lanes), f32),
            pltpu.VMEM((2, 2, nx, lanes), f32),
            pltpu.VMEM((2, groups, 8, lanes), f32),
            pltpu.VMEM((2, 2, groups, 8, lanes), f32),
            pltpu.SemaphoreType.DMA((4,)),
            pltpu.SemaphoreType.DMA((2, 8)),
            pltpu.SemaphoreType.DMA((2, 8)),
        ],
        compiler_params=pltpu.CompilerParams(collective_id=hops, has_side_effects=True),
    )(shear, conc, speed, signs, diff)


def body(concentration, speed, signs, diffusivity, shear):
    counts = tuple(lax.axis_size(name) for name in ("gx", "gy", "gz"))
    rows = concentration.shape[1]
    branches = [functools.partial(run, hops, counts) for hops in range(counts[1])]
    return lax.switch(
        lax.div(shear[0], rows), branches, shear, concentration, speed, signs, diffusivity
    )


def solution(mesh):
    placed = (
        P("gx", "gy", "gz"),
        P(None, "gx", "gy", "gz"),
        P(None, "gx", "gy", "gz"),
        P("gx", "gy", "gz"),
        P(),
    )
    return jax.shard_map(
        body, mesh=mesh, in_specs=placed, out_specs=P("gx", "gy", "gz"), check_vma=False
    )
```

```python
import functools

import jax
import jax.numpy as jnp
from jax import lax
from jax.experimental import pallas as pl
from jax.experimental.pallas import tpu as pltpu
from jax.sharding import PartitionSpec as P

STEPS = 8
time_step = 0.25
PAD = 8
MESH = pl.DeviceIdType.MESH


def kernel(
    hops, count_x, count_y, count_z,
    shear, conc, speed, signs, diff, out,
    field0, field1, coef, v_buf, s_buf, d_buf, low0, low1, high0, high1,
    y_out0, y_out1, y_in0, y_in1, z_out0, z_out1, z_in0, z_in1,
    load_sem, send_sem, recv_sem,
):
    nx, rows, lanes = conc.shape
    blocks = rows // 8
    span = 2 * nx
    per = lanes // span
    gx, gy, gz = (lax.axis_index(name) for name in ("gx", "gy", "gz"))
    low, high, field = (low0, low1), (high0, high1), (field0, field1)
    y_out, y_in = (y_out0, y_out1), (y_in0, y_in1)
    z_out, z_in = (z_out0, z_out1), (z_in0, z_in1)
    first, last = gx == 0, gx == count_x - 1
    body_rows = pl.ds(PAD, rows)

    def at(x, y):
        return {"gx": x, "gy": lax.rem(y + 2 * count_y, count_y)}

    up = (
        at(jnp.where(last, 0, gx + 1), gy - jnp.where(last, hops, 0)),
        at(0, gy - hops - 1),
    )
    down = (
        at(jnp.where(first, count_x - 1, gx - 1), gy + jnp.where(first, hops + 1, 0)),
        at(count_x - 1, gy + hops),
    )
    before_y, after_y = at(gx, gy - 1), at(gx, gy + 1)
    before_z = {"gz": lax.rem(gz + count_z - 1, count_z)}
    after_z = {"gz": lax.rem(gz + 1, count_z)}

    def remote(p, role, source, target, device):
        return pltpu.make_async_remote_copy(
            src_ref=source, dst_ref=target,
            send_sem=send_sem.at[p, role], recv_sem=recv_sem.at[p, role],
            device_id=device, device_id_type=MESH,
        )

    def copies(p):
        top = field[p].at[nx - 1, body_rows]
        bottom = field[p].at[0, body_rows]
        halves = (pl.ds(0, rows), pl.ds(rows, rows))
        return (
            remote(p, 0, top, low[p].at[halves[0]], up[0]),
            remote(p, 1, top, low[p].at[halves[1]], up[1]),
            remote(p, 2, bottom, high[p].at[halves[0]], down[0]),
            remote(p, 3, bottom, high[p].at[halves[1]], down[1]),
            remote(p, 4, y_out[p].at[0], y_in[p].at[1], before_y),
            remote(p, 5, y_out[p].at[1], y_in[p].at[0], after_y),
            remote(p, 6, z_out[p], z_in[p].at[1], before_z),
            remote(p, 7, z_out[p], z_in[p].at[0], after_z),
        )

    def send(p):
        c = copies(p)
        pl.when(last)(c[1].start)
        pl.when(first)(c[3].start)
        for role in (0, 2, 4, 5, 6, 7):
            c[role].start()

    lane = lax.broadcasted_iota(jnp.int32, (8, lanes), 1)
    even = lane % 2 == 0

    def turn(value, amount):
        amount = amount % lanes
        return pltpu.roll(value, amount, 1) if amount else value

    def record(q, packed, block, x, value):
        spot = span * (block % per) + 2 * x
        group = block // per
        moved = turn(value, spot + 1)
        packed[group] = jnp.where((lane == spot) | (lane == spot + 1), moved, packed[group])
        if block == 0:
            y_out[q][0, pl.ds(x, 1)] = value[:1]
        if block == blocks - 1:
            y_out[q][1, pl.ds(x, 1)] = value[7:]

    def store_packed(q, packed):
        for group, value in enumerate(packed):
            z_out[q][group] = value

    groups = blocks // per
    def nothing():
        return [jnp.zeros((8, lanes), jnp.float32) for _ in range(groups)]


    loads = (
        pltpu.make_async_copy(conc, field[0].at[:, body_rows], load_sem.at[0]),
        pltpu.make_async_copy(diff, d_buf, load_sem.at[1]),
        pltpu.make_async_copy(speed, v_buf, load_sem.at[2]),
        pltpu.make_async_copy(signs, s_buf, load_sem.at[3]),
    )
    for load in loads:
        load.start()

    barrier = pltpu.get_barrier_semaphore()

    def greet(device):
        pl.semaphore_signal(barrier, inc=1, device_id=device, device_id_type=MESH)

    for device in (up[0], down[0], before_y, after_y, before_z, after_z):
        greet(device)
    pl.when(last)(lambda: greet(up[1]))
    pl.when(first)(lambda: greet(down[1]))
    pl.semaphore_wait(barrier, 6 + jnp.where(first | last, 1, 0))

    loads[0].wait()

    packed = nothing()
    for block in range(blocks):
        for x in range(nx):
            record(0, packed, block, x, field[0][x, pl.ds(PAD + 8 * block, 8)])
    store_packed(0, packed)
    send(0)
    for load in loads[1:]:
        load.wait()

    def weigh(x, carry):
        d = time_step * d_buf[x]
        centre = 1.0 - 6.0 * d
        for axis in range(3):
            v = time_step * v_buf[axis, x]
            forward = s_buf[axis, x] > 0
            below = jnp.where(forward, v, 0.0)
            above = v - below
            coef[1 + 2 * axis, x] = d + below
            coef[2 + 2 * axis, x] = d - above
            centre = centre - below + above
        coef[0, x] = centre
        return carry

    lax.fori_loop(0, nx, weigh, 0)

    residue = lax.rem(shear[0], rows)
    low_start = jnp.where(first, residue, 0)
    high_start = jnp.where(last, rows - residue, 0)

    def step(p, more):
        q = 1 - p
        c = copies(p)
        old, new = field[p], field[q]
        c[6].wait_recv()
        c[7].wait_recv()
        sides = [
            jnp.where(even, z_in[p][0, group], turn(z_in[p][1, group], -2))
            for group in range(groups)
        ]
        packed = nothing()

        def cells(block, x, lower, here, upper):
            start = PAD + 8 * block
            part = pl.ds(8 * block, 8)
            side = turn(sides[block // per], -(span * (block % per) + 2 * x))
            z_minus = jnp.where(lane == 0, side, turn(here, 1))
            z_plus = jnp.where(lane == lanes - 1, side, turn(here, -1))
            total = (
                (coef[0, x, part] * here + coef[1, x, part] * lower)
                + (coef[2, x, part] * upper
                   + coef[3, x, part] * old[x, pl.ds(start - 1, 8)])
            ) + (
                (coef[4, x, part] * old[x, pl.ds(start + 1, 8)]
                 + coef[5, x, part] * z_minus)
                + coef[6, x, part] * z_plus
            )
            new[x, pl.ds(start, 8)] = total
            record(q, packed, block, x, total)

        def column(block):
            at_x = lambda x: old[x, pl.ds(PAD + 8 * block, 8)]
            lower, here = at_x(0), at_x(1)
            for x in range(1, nx - 1):
                upper = at_x(x + 1)
                cells(block, x, lower, here, upper)
                lower, here = here, upper

        for block in range(1, blocks - 1):
            column(block)
        c[4].wait_recv()
        c[5].wait_recv()
        for x in range(nx):
            old[x, pl.ds(PAD - 1, 1)] = y_in[p][0, pl.ds(x, 1)]
            old[x, pl.ds(PAD + rows, 1)] = y_in[p][1, pl.ds(x, 1)]
        column(0)
        column(blocks - 1)
        c[0].wait_recv()
        c[2].wait_recv()
        pl.when(first)(c[1].wait_recv)
        pl.when(last)(c[3].wait_recv)
        for block in range(blocks):
            at_x = lambda x: old[x, pl.ds(PAD + 8 * block, 8)]
            cells(block, 0, low[p][pl.ds(low_start + 8 * block, 8)], at_x(0), at_x(1))
            cells(block, nx - 1, at_x(nx - 2), at_x(nx - 1), high[p][pl.ds(high_start + 8 * block, 8)])
        store_packed(q, packed)
        for role in (0, 2, 4, 5, 6, 7):
            c[role].wait_send()
        pl.when(last)(c[1].wait_send)
        pl.when(first)(c[3].wait_send)
        if more is None:
            send(q)
        else:
            pl.when(more)(lambda: send(q))

    def pair(t, carry):
        step(0, None)
        step(1, t < STEPS // 2 - 1)
        return carry

    lax.fori_loop(0, STEPS // 2, pair, 0)
    store = pltpu.make_async_copy(field[STEPS % 2].at[:, body_rows], out, load_sem.at[0])
    store.start()
    store.wait()


def run(hops, counts, shear, conc, speed, signs, diff):
    nx, rows, lanes = conc.shape
    f32 = jnp.float32
    groups = (rows // 8) // (lanes // (2 * nx))
    anywhere = pl.BlockSpec(memory_space=pl.ANY)
    return pl.pallas_call(
        functools.partial(kernel, hops, *counts),
        name=f"slide{hops}",
        out_shape=jax.ShapeDtypeStruct(conc.shape, f32),
        in_specs=[pl.BlockSpec(memory_space=pltpu.SMEM)] + [anywhere] * 4,
        out_specs=anywhere,
        scratch_shapes=[
            pltpu.VMEM((nx, rows + 2 * PAD, lanes), f32),
            pltpu.VMEM((nx, rows + 2 * PAD, lanes), f32),
            pltpu.VMEM((7, nx, rows, lanes), f32),
            pltpu.VMEM((3, nx, rows, lanes), f32),
            pltpu.VMEM((3, nx, rows, lanes), jnp.int32),
            pltpu.VMEM((nx, rows, lanes), f32),
            pltpu.VMEM((2 * rows, lanes), f32),
            pltpu.VMEM((2 * rows, lanes), f32),
            pltpu.VMEM((2 * rows, lanes), f32),
            pltpu.VMEM((2 * rows, lanes), f32),
            *[pltpu.VMEM((2, nx, lanes), f32)] * 4,
            *[pltpu.VMEM((groups, 8, lanes), f32)] * 2,
            *[pltpu.VMEM((2, groups, 8, lanes), f32)] * 2,
            pltpu.SemaphoreType.DMA((4,)),
            pltpu.SemaphoreType.DMA((2, 8)),
            pltpu.SemaphoreType.DMA((2, 8)),
        ],
        compiler_params=pltpu.CompilerParams(collective_id=hops, has_side_effects=True),
    )(shear, conc, speed, signs, diff)


def body(concentration, speed, signs, diffusivity, shear):
    counts = tuple(lax.axis_size(name) for name in ("gx", "gy", "gz"))
    rows = concentration.shape[1]
    branches = [functools.partial(run, hops, counts) for hops in range(counts[1])]
    return lax.switch(
        lax.div(shear[0], rows), branches, shear, concentration, speed, signs, diffusivity
    )


def solution(mesh):
    placed = (
        P("gx", "gy", "gz"),
        P(None, "gx", "gy", "gz"),
        P(None, "gx", "gy", "gz"),
        P("gx", "gy", "gz"),
        P(),
    )
    return jax.shard_map(
        body, mesh=mesh, in_specs=placed, out_specs=P("gx", "gy", "gz"), check_vma=False
    )
```

```python
import functools

import jax
import jax.numpy as jnp
from jax import lax
from jax.experimental import pallas as pl
from jax.experimental.pallas import tpu as pltpu
from jax.sharding import PartitionSpec as P

STEPS = 8
time_step = 0.25
PAD = 8
MESH = pl.DeviceIdType.MESH


def kernel(
    hops, count_x, count_y, count_z,
    shear, conc, speed, signs, diff, out,
    field0, field1, coef, v_buf, s_buf, d_buf, low0, low1, high0, high1,
    y_out0, y_out1, y_in0, y_in1, z_out0, z_out1, z_in0, z_in1,
    load_sem, send_sem, recv_sem,
):
    nx, rows, lanes = conc.shape
    blocks = rows // 8
    span = 2 * nx
    per = lanes // span
    gx, gy, gz = (lax.axis_index(name) for name in ("gx", "gy", "gz"))
    low, high, field = (low0, low1), (high0, high1), (field0, field1)
    y_out, y_in = (y_out0, y_out1), (y_in0, y_in1)
    z_out, z_in = (z_out0, z_out1), (z_in0, z_in1)
    first, last = gx == 0, gx == count_x - 1
    body_rows = pl.ds(PAD, rows)

    def at(x, y):
        return {"gx": x, "gy": lax.rem(y + 2 * count_y, count_y)}

    up = (
        at(jnp.where(last, 0, gx + 1), gy - jnp.where(last, hops, 0)),
        at(0, gy - hops - 1),
    )
    down = (
        at(jnp.where(first, count_x - 1, gx - 1), gy + jnp.where(first, hops + 1, 0)),
        at(count_x - 1, gy + hops),
    )
    before_y, after_y = at(gx, gy - 1), at(gx, gy + 1)
    before_z = {"gz": lax.rem(gz + count_z - 1, count_z)}
    after_z = {"gz": lax.rem(gz + 1, count_z)}

    def remote(p, role, source, target, device):
        return pltpu.make_async_remote_copy(
            src_ref=source, dst_ref=target,
            send_sem=send_sem.at[p, role], recv_sem=recv_sem.at[p, role],
            device_id=device, device_id_type=MESH,
        )

    def copies(p):
        top = field[p].at[nx - 1, body_rows]
        bottom = field[p].at[0, body_rows]
        halves = (pl.ds(0, rows), pl.ds(rows, rows))
        return (
            remote(p, 0, top, low[p].at[halves[0]], up[0]),
            remote(p, 1, top, low[p].at[halves[1]], up[1]),
            remote(p, 2, bottom, high[p].at[halves[0]], down[0]),
            remote(p, 3, bottom, high[p].at[halves[1]], down[1]),
            remote(p, 4, y_out[p].at[0], y_in[p].at[1], before_y),
            remote(p, 5, y_out[p].at[1], y_in[p].at[0], after_y),
            remote(p, 6, z_out[p], z_in[p].at[1], before_z),
            remote(p, 7, z_out[p], z_in[p].at[0], after_z),
        )

    def send(p):
        c = copies(p)
        for role in (6, 7, 4, 5):
            c[role].start()
        pl.when(last)(c[1].start)
        pl.when(first)(c[3].start)
        c[0].start()
        c[2].start()

    lane = lax.broadcasted_iota(jnp.int32, (8, lanes), 1)
    even = lane % 2 == 0

    def turn(value, amount):
        amount = amount % lanes
        return pltpu.roll(value, amount, 1) if amount else value

    def record(q, packed, block, x, value):
        spot = span * (block % per) + 2 * x
        group = block // per
        moved = turn(value, spot + 1)
        packed[group] = jnp.where((lane == spot) | (lane == spot + 1), moved, packed[group])
        if block == 0:
            y_out[q][0, pl.ds(x, 1)] = value[:1]
        if block == blocks - 1:
            y_out[q][1, pl.ds(x, 1)] = value[7:]

    def store_packed(q, packed):
        for group, value in enumerate(packed):
            z_out[q][group] = value

    groups = blocks // per
    def nothing():
        return [jnp.zeros((8, lanes), jnp.float32) for _ in range(groups)]


    loads = (
        pltpu.make_async_copy(conc, field[0].at[:, body_rows], load_sem.at[0]),
        pltpu.make_async_copy(diff, d_buf, load_sem.at[1]),
        pltpu.make_async_copy(speed, v_buf, load_sem.at[2]),
        pltpu.make_async_copy(signs, s_buf, load_sem.at[3]),
    )
    for load in loads:
        load.start()

    barrier = pltpu.get_barrier_semaphore()

    def greet(device):
        pl.semaphore_signal(barrier, inc=1, device_id=device, device_id_type=MESH)

    for device in (up[0], down[0], before_y, after_y, before_z, after_z):
        greet(device)
    pl.when(last)(lambda: greet(up[1]))
    pl.when(first)(lambda: greet(down[1]))
    pl.semaphore_wait(barrier, 6 + jnp.where(first | last, 1, 0))

    loads[0].wait()

    packed = nothing()
    for block in range(blocks):
        for x in range(nx):
            record(0, packed, block, x, field[0][x, pl.ds(PAD + 8 * block, 8)])
    store_packed(0, packed)
    send(0)
    for load in loads[1:]:
        load.wait()

    def weigh(x, carry):
        d = time_step * d_buf[x]
        centre = 1.0 - 6.0 * d
        for axis in range(3):
            v = time_step * v_buf[axis, x]
            forward = s_buf[axis, x] > 0
            below = jnp.where(forward, v, 0.0)
            above = v - below
            coef[1 + 2 * axis, x] = d + below
            coef[2 + 2 * axis, x] = d - above
            centre = centre - below + above
        coef[0, x] = centre
        return carry

    lax.fori_loop(0, nx, weigh, 0)

    residue = lax.rem(shear[0], rows)
    low_start = jnp.where(first, residue, 0)
    high_start = jnp.where(last, rows - residue, 0)

    def step(p, more):
        q = 1 - p
        c = copies(p)
        old, new = field[p], field[q]
        c[6].wait_recv()
        c[7].wait_recv()
        sides = [
            jnp.where(even, z_in[p][0, group], turn(z_in[p][1, group], -2))
            for group in range(groups)
        ]
        packed = nothing()

        def cells(block, x, lower, here, upper):
            start = PAD + 8 * block
            part = pl.ds(8 * block, 8)
            side = turn(sides[block // per], -(span * (block % per) + 2 * x))
            z_minus = jnp.where(lane == 0, side, turn(here, 1))
            z_plus = jnp.where(lane == lanes - 1, side, turn(here, -1))
            total = (
                (coef[0, x, part] * here + coef[1, x, part] * lower)
                + (coef[2, x, part] * upper
                   + coef[3, x, part] * old[x, pl.ds(start - 1, 8)])
            ) + (
                (coef[4, x, part] * old[x, pl.ds(start + 1, 8)]
                 + coef[5, x, part] * z_minus)
                + coef[6, x, part] * z_plus
            )
            new[x, pl.ds(start, 8)] = total
            record(q, packed, block, x, total)

        def column(block):
            at_x = lambda x: old[x, pl.ds(PAD + 8 * block, 8)]
            lower, here = at_x(0), at_x(1)
            for x in range(1, nx - 1):
                upper = at_x(x + 1)
                cells(block, x, lower, here, upper)
                lower, here = here, upper

        for block in range(1, blocks - 1):
            column(block)
        c[4].wait_recv()
        c[5].wait_recv()
        for x in range(nx):
            old[x, pl.ds(PAD - 1, 1)] = y_in[p][0, pl.ds(x, 1)]
            old[x, pl.ds(PAD + rows, 1)] = y_in[p][1, pl.ds(x, 1)]
        column(0)
        column(blocks - 1)
        for role in (0, 2, 4, 5, 6, 7):
            c[role].wait_send()
        pl.when(last)(c[1].wait_send)
        pl.when(first)(c[3].wait_send)
        c[0].wait_recv()
        c[2].wait_recv()
        pl.when(first)(c[1].wait_recv)
        pl.when(last)(c[3].wait_recv)
        for block in range(blocks):
            at_x = lambda x: old[x, pl.ds(PAD + 8 * block, 8)]
            cells(block, 0, low[p][pl.ds(low_start + 8 * block, 8)], at_x(0), at_x(1))
            cells(block, nx - 1, at_x(nx - 2), at_x(nx - 1), high[p][pl.ds(high_start + 8 * block, 8)])
        store_packed(q, packed)
        if more is None:
            send(q)
        else:
            pl.when(more)(lambda: send(q))

    def pair(t, carry):
        step(0, None)
        step(1, t < STEPS // 2 - 1)
        return carry

    lax.fori_loop(0, STEPS // 2, pair, 0)
    store = pltpu.make_async_copy(field[STEPS % 2].at[:, body_rows], out, load_sem.at[0])
    store.start()
    store.wait()


def run(hops, counts, shear, conc, speed, signs, diff):
    nx, rows, lanes = conc.shape
    f32 = jnp.float32
    groups = (rows // 8) // (lanes // (2 * nx))
    anywhere = pl.BlockSpec(memory_space=pl.ANY)
    return pl.pallas_call(
        functools.partial(kernel, hops, *counts),
        name=f"slide{hops}",
        out_shape=jax.ShapeDtypeStruct(conc.shape, f32),
        in_specs=[pl.BlockSpec(memory_space=pltpu.SMEM)] + [anywhere] * 4,
        out_specs=anywhere,
        scratch_shapes=[
            pltpu.VMEM((nx, rows + 2 * PAD, lanes), f32),
            pltpu.VMEM((nx, rows + 2 * PAD, lanes), f32),
            pltpu.VMEM((7, nx, rows, lanes), f32),
            pltpu.VMEM((3, nx, rows, lanes), f32),
            pltpu.VMEM((3, nx, rows, lanes), jnp.int32),
            pltpu.VMEM((nx, rows, lanes), f32),
            pltpu.VMEM((2 * rows, lanes), f32),
            pltpu.VMEM((2 * rows, lanes), f32),
            pltpu.VMEM((2 * rows, lanes), f32),
            pltpu.VMEM((2 * rows, lanes), f32),
            *[pltpu.VMEM((2, nx, lanes), f32)] * 4,
            *[pltpu.VMEM((groups, 8, lanes), f32)] * 2,
            *[pltpu.VMEM((2, groups, 8, lanes), f32)] * 2,
            pltpu.SemaphoreType.DMA((4,)),
            pltpu.SemaphoreType.DMA((2, 8)),
            pltpu.SemaphoreType.DMA((2, 8)),
        ],
        compiler_params=pltpu.CompilerParams(collective_id=hops, has_side_effects=True),
    )(shear, conc, speed, signs, diff)


def body(concentration, speed, signs, diffusivity, shear):
    counts = tuple(lax.axis_size(name) for name in ("gx", "gy", "gz"))
    rows = concentration.shape[1]
    branches = [functools.partial(run, hops, counts) for hops in range(counts[1])]
    return lax.switch(
        lax.div(shear[0], rows), branches, shear, concentration, speed, signs, diffusivity
    )


def solution(mesh):
    placed = (
        P("gx", "gy", "gz"),
        P(None, "gx", "gy", "gz"),
        P(None, "gx", "gy", "gz"),
        P("gx", "gy", "gz"),
        P(),
    )
    return jax.shard_map(
        body, mesh=mesh, in_specs=placed, out_specs=P("gx", "gy", "gz"), check_vma=False
    )
```
